32 devices in a mesh: scen: 8 (over y, x, core), own: 4 (over z).
Axes of the slice: x: 2, y: 2, z: 4, core: 2. Of those that a mesh axis runs over, the one named last changes fastest.
Arguments:
- returns: float32 [8192, 4096], P('scen', 'own'), may hold values from -50 to 50, as said below
Outputs:
- shrunk_cov: float32 [4096, 4096], P('scen', 'own')
The draws below stay inside these ranges and needn't reach their ends.
Inputs may be any that keep to these rules, and one draw needn't show every extreme that they name: Finite real returns.
All inputs are finite; a program needn't handle non-finite values.
Results may differ from the reference program's by a relative error of at most 0.00014.
Values sent between devices are 32-bit elements; how exact they have to be, the bound alone decides.
A program may use at most 128 MiB of HBM per device.

```python
import jax
import jax.numpy as jnp
from jax import lax

P_SIZE = 4096
SCENARIOS = 8192


def draw_returns(key, part):
    keys = jax.random.split(key, 6)
    factor_pos = jnp.arange(P_SIZE, dtype=jnp.float32) / P_SIZE
    scen_pos = jnp.arange(SCENARIOS, dtype=jnp.float32) / SCENARIOS
    col_jitter = jax.random.uniform(keys[0], (P_SIZE,), jnp.float32)
    row_jitter = jax.random.uniform(keys[1], (SCENARIOS,), jnp.float32)
    col_scale = 0.1 * 10.0 ** (factor_pos + 0.3 * (col_jitter - 0.5))
    row_scale = 4.0 ** scen_pos * jnp.exp(0.2 * (row_jitter - 0.5))
    noise = jax.random.normal(keys[2], (SCENARIOS, P_SIZE), jnp.float32)
    offsets = 0.5 * col_scale * jax.random.normal(keys[5], (P_SIZE,), jnp.float32)
    values = row_scale[:, None] * col_scale[None, :] * noise + offsets[None, :]
    return jnp.clip(values, -50.0, 50.0).astype(jnp.float32)


def setup_inputs(seed: int = 0) -> dict:
    seeds = jax.random.split(jax.random.key(seed), 2)
    returns = draw_returns(jax.random.fold_in(seeds[1], 71), 0)
    return dict(returns=returns)


epsilon = 1e-6


def reference(returns):
    scenarios = returns.shape[0]
    order = returns.shape[1]
    col_mean = jnp.sum(returns, axis=0) / scenarios
    centered = returns - col_mean
    gram = lax.dot_general(centered, centered, (((0,), (0,)), ((), ())), precision=lax.Precision.HIGHEST, preferred_element_type=jnp.float32)
    covariance = gram / scenarios
    squares = centered * centered
    trace_sum = jnp.sum(squares)
    row_norm = jnp.sum(squares, axis=1)
    beta_raw = jnp.sum(row_norm * row_norm)
    frob_sum = jnp.sum(covariance * covariance)
    target = trace_sum / (scenarios * order)
    beta_term = (beta_raw / scenarios - frob_sum) / (order * scenarios)
    delta_term = (frob_sum - order * target * target) / order
    shrinkage = beta_term / (delta_term + epsilon)
    row_ids = lax.broadcasted_iota(jnp.int32, (order, order), 0)
    col_ids = lax.broadcasted_iota(jnp.int32, (order, order), 1)
    diag_mask = (row_ids == col_ids).astype(jnp.float32)
    return (1.0 - shrinkage) * covariance + shrinkage * target * diag_mask
```

```python
import jax
import jax.numpy as jnp
from jax import lax
from jax.sharding import PartitionSpec as P

epsilon = 1e-06
CHUNKS = 2


def product_over_scenarios(left_part, right_part):
    return lax.dot_general(
        left_part,
        right_part,
        (((0,), (0,)), ((), ())),
        precision=lax.Precision.HIGH,
        preferred_element_type=jnp.float32,
    )


def gram_of(left, right):
    return jnp.stack([product_over_scenarios(part, right) for part in left])


def pick(parts, index, axis):
    return lax.dynamic_index_in_dim(parts, index, axis, keepdims=False)


def exchange_bit(sent, bit, scen_devices):
    return lax.ppermute(sent, "scen", [(s, s ^ (1 << bit)) for s in range(scen_devices)])


def halve(parts, order, me, scen_devices):
    left = sorted(order, reverse=True)
    for bit in order:
        axis = left.index(bit)
        mine = (me >> bit) & 1
        got = exchange_bit(pick(parts, 1 - mine, axis), bit, scen_devices)
        parts = pick(parts, mine, axis) + got
        left.remove(bit)
    return parts


def on_device(returns):
    scen_devices = lax.axis_size("scen")
    own_devices = lax.axis_size("own")
    me = lax.axis_index("scen")
    plane = lax.axis_index("own")
    local_rows, own_cols = returns.shape
    scenarios = local_rows * scen_devices
    order = own_cols * own_devices
    group = scen_devices // own_devices
    height = order // scen_devices
    bits = scen_devices.bit_length() - 1
    half = local_rows // 2
    chunks = max(1, min(CHUNKS, height // 128))
    width = height // chunks

    col_mean = lax.psum(jnp.sum(returns, axis=0), "scen") / scenarios
    centered = returns - col_mean
    halves = centered.reshape(2, half, own_cols)
    split = centered.reshape(2, half, group, chunks, width).transpose(3, 0, 2, 1, 4)
    upward = [(z, z + 1) for z in range(own_devices - 1)]
    downward = [(z + 1, z) for z in range(own_devices - 1)]
    low_bit = me & 1
    mid = own_cols // 2
    high_bits = list(range(1, bits))
    tile_chunks = []
    gate = None
    for c in range(chunks):
        up, down = split[c, 0], split[c, 1]
        if gate is not None:
            up, down, _ = lax.optimization_barrier((up, down, gate))
        ups, downs = [up], [down]
        for step in range(1, own_devices):
            up = lax.ppermute(up, "own", upward)
            down = lax.ppermute(down, "own", downward)
            ups.append(up)
            downs.append(down)
            if step == own_devices - 2:
                gate = (up[0, :8, :128], down[0, :8, :128])

        def strip(side):
            blocks = []
            for d in range(own_devices):
                if d == 0:
                    left = pick(
                        split[c].reshape(2, group // 2, 2, half, width), side, 2
                    )
                    block = sum(
                        gram_of(left[e], halves[e]) for e in range(2)
                    )
                else:
                    above = plane + d < own_devices
                    left = jnp.where(above, downs[d], ups[own_devices - d])
                    left = pick(left.reshape(group // 2, 2, half, width), side, 1)
                    block = gram_of(left, pick(halves, above.astype(jnp.int32), 0))
                blocks.append(block)
            return jnp.stack(blocks)

        got = exchange_bit(strip(1 - low_bit), 0, scen_devices)
        rel = strip(low_bit) + got
        parts = jnp.stack(
            [pick(rel, (i - plane) % own_devices, 0) for i in range(own_devices)]
        )
        parts = parts.reshape((2,) * (bits - 1) + (width, own_cols))
        first = halve(parts[..., :mid], high_bits, me, scen_devices)
        second = halve(parts[..., mid:], high_bits[::-1], me, scen_devices)
        tile_chunks.append(jnp.concatenate([first, second], axis=1))

    squares = centered * centered
    norm_part = jnp.sum(squares, axis=1)
    row_norm = lax.psum(norm_part, "own")
    trace_local = jnp.sum(norm_part)
    beta_local = jnp.sum(row_norm * row_norm) / own_devices

    my_part = me % group
    tile = jnp.concatenate(tile_chunks, axis=0) if chunks > 1 else tile_chunks[0]
    columns = []
    received = []
    for k in range(group):
        pairs = []
        for i in range(own_devices):
            for h in range(group):
                for j in range(own_devices):
                    if i != j:
                        source = (i * group + h) * own_devices + j
                        target = (j * group + (h + k) % group) * own_devices + i
                        pairs.append((source, target))
        fetched = []
        for c in range(chunks):
            piece = pick(
                tile_chunks[c].reshape(width, group, height), (my_part + k) % group, 1
            )
            fetched.append(lax.ppermute(piece, ("scen", "own"), pairs))
        received.append(jnp.concatenate(fetched, axis=0).T)
    stacked = jnp.stack(received)
    for h in range(group):
        columns.append(pick(stacked, (my_part - h) % group, 0))
    covariance = (tile + jnp.concatenate(columns, axis=1)) / scenarios

    sums = jnp.stack([jnp.sum(covariance * covariance), trace_local, beta_local])
    frob_sum, trace_sum, beta_raw = lax.psum(lax.psum(sums, "own"), "scen")
    target = trace_sum / (scenarios * order)
    beta_term = (beta_raw / scenarios - frob_sum) / (order * scenarios)
    delta_term = (frob_sum - order * target * target) / order
    shrinkage = beta_term / (delta_term + epsilon)
    row_ids = me * height + lax.broadcasted_iota(jnp.int32, covariance.shape, 0)
    col_ids = plane * own_cols + lax.broadcasted_iota(jnp.int32, covariance.shape, 1)
    diag_mask = (row_ids == col_ids).astype(jnp.float32)
    return (1.0 - shrinkage) * covariance + shrinkage * target * diag_mask


def solution(mesh):
    placed = (P("scen", "own"),)
    return jax.shard_map(
        on_device, mesh=mesh, in_specs=placed, out_specs=P("scen", "own"), check_vma=False
    )
```
